256 devices in a mesh: groups: 2 (over y), rows: 16 (over z), sub: 8 (over x, core).
Axes of the slice: x: 4, y: 2, z: 16, core: 2. Of those that a mesh axis runs over, the one named last changes fastest.
The devices are a block of a 4x16x16 slice.
Arguments:
- matrix: float32 [131072, 1024], P(('groups', 'rows', 'sub')), parts along dimension 0
- sign_bits: int32 [131072], P(('groups', 'rows', 'sub')), parts along dimension 0, may hold values from 0 to 1
- samples: int32 [8192], P('groups'), parts along dimension 0, may hold values from 0 to 65535
Outputs:
- cholesky_factor: float32 [2048, 1024], P('groups'), parts along dimension 0
The draws below stay inside these ranges and needn't reach their ends.
There are 2 independent parts, one for each index of `groups`. The reference program is written for one: setup_inputs(seed, part) draws one part's arguments, and reference() takes and returns one part's arrays. A program takes and returns all parts, laid end to end along the dimension named above; each array names one. Nothing has to cross between parts.
Inputs may be any that keep to these rules, and one draw needn't show every extreme that they name: `samples`: row numbers of the whole matrix, drawn independently; a row may be drawn more than once.
All inputs are finite; a program needn't handle non-finite values.
Results may differ from the reference program's by a relative error of at most 0.00011.
Values sent between devices are 32-bit elements; how exact they have to be, the bound alone decides.
A program may use at most 64 MiB of HBM per device.

```python
import math
import jax
import jax.numpy as jnp
from jax import lax

N = 1024
S = 4096
M = 65536


def draw_matrix(key, part):
    streams = jax.random.split(jax.random.fold_in(key, 17), 3)
    column_scale = jnp.exp(jax.random.uniform(streams[0], (N,), jnp.float32, 0.0, math.log(3.0)))
    row_scale = jnp.exp(jax.random.uniform(streams[1], (M,), jnp.float32, 0.0, math.log(10.0)))
    raw_values = jax.random.truncated_normal(streams[2], -6.0, 6.0, (M, N), jnp.float32)
    return raw_values * row_scale[:, None] * column_scale[None, :] * 0.25


def place_ends(result, own_key, low, largest):
    longest = result.shape.index(max(result.shape))
    spots = []
    for shift in (0, 1):
        where = [jax.random.randint(jax.random.fold_in(own_key, axis), (), 0, length) for axis, length in enumerate(result.shape)]
        where[longest] = (where[longest] + shift) % result.shape[longest]
        spots.append(tuple(where))
    return result.at[spots[0]].set(low).at[spots[1]].set(largest)


def setup_inputs(seed: int = 0, part: int = 0) -> dict:
    arg_keys = jax.random.split(jax.random.key(seed), 4)
    part_keys = jax.random.split(jax.random.fold_in(arg_keys[3], part), 4)
    matrix = draw_matrix(jax.random.fold_in(jax.random.fold_in(arg_keys[3], part), 71), part)
    sign_bits = place_ends(jax.random.randint(part_keys[1], (M,), 0, 2), jax.random.fold_in(part_keys[1], 1), 0, 1).astype(jnp.int32)
    samples = place_ends(jax.random.randint(part_keys[2], (S,), 0, M), jax.random.fold_in(part_keys[2], 1), 0, M - 1).astype(jnp.int32)
    return {"matrix": matrix, "sign_bits": sign_bits, "samples": samples}


def hadamard_rows(values):
    extent = values.shape[0]
    columns = values.shape[1]
    stride = 1
    for level in range(extent.bit_length() - 1):
        paired = values.reshape(extent // (2 * stride), 2, stride, columns)
        values = jnp.stack((paired[:, 0] + paired[:, 1], paired[:, 0] - paired[:, 1]), axis=1).reshape(extent, columns)
        stride = stride * 2
    return values

def reference(matrix, sign_bits, samples):
    sign_values = (2 * sign_bits - 1).astype(jnp.float32)
    signed = matrix * sign_values[:, None]
    mixed_rows = hadamard_rows(signed) / jnp.sqrt(jnp.float32(matrix.shape[0]))
    picked = jnp.take(mixed_rows, samples.astype(jnp.int32), axis=0)
    gram_matrix = jnp.dot(picked.T.astype(jnp.float32), picked.astype(jnp.float32), precision=lax.Precision.HIGHEST, preferred_element_type=jnp.float32) / jnp.float32(samples.shape[0])
    return jnp.linalg.cholesky(gram_matrix)
```

```python
import functools

import jax
import jax.numpy as jnp
from jax import lax
from jax.experimental import pallas as pl
from jax.experimental.pallas import tpu as pltpu
from jax.sharding import Mesh
from jax.sharding import PartitionSpec as P

GROUPS_ROWS_SUB = ("groups", "rows", "sub_0", "sub_1")
BLK = 128
SUB = 32
SUB0 = 4
SLOTS = 5
PIECES = 2
F32 = jnp.float32
BF = jnp.bfloat16


def row_of(vec, s):
    return jnp.broadcast_to(vec[s:s + 1, :], vec.shape)


def split(x):
    hi = x.astype(BF)
    return hi, (x - hi.astype(F32)).astype(BF)


def dot3(ah, al, bh, bl):
    d = functools.partial(jnp.dot, preferred_element_type=F32)
    return d(ah, bh) + (d(ah, bl) + d(al, bh))


def factor_diagonal(w, u):
    for p in range(BLK // SUB):
        r0 = SUB * p
        ngrp = SUB // 8
        sl = [slice(r0 + 8 * g, r0 + 8 * g + 8) for g in range(ngrp)]
        ta = [w[sl[g], 0:BLK] for g in range(ngrp)]
        te = [w[sl[g], BLK:2 * BLK] for g in range(ngrp)]
        cols = {}
        for c in range(SUB):
            for g in range(c // 8, ngrp):
                cols[c, g] = jnp.broadcast_to(ta[g][:, r0 + c:r0 + c + 1], (8, BLK))
        for i in range(SUB):
            g, s = divmod(i, 8)
            r = lax.rsqrt(row_of(cols[i, g], s))
            lo = {h: cols[i, h] * r for h in range(g, ngrp)}
            ua = row_of(ta[g], s) * r
            ue = row_of(te[g], s) * r
            u[r0 + i:r0 + i + 1, 0:BLK] = ua[0:1]
            u[r0 + i:r0 + i + 1, BLK:2 * BLK] = ue[0:1]
            for c in range(i + 1, SUB):
                m = row_of(lo[c // 8], c % 8)
                for h in range(c // 8, ngrp):
                    cols[c, h] = cols[c, h] - lo[h] * m
            for h in range(g, ngrp):
                if h > g or s < 7:
                    ta[h] = ta[h] - lo[h] * ua
                    te[h] = te[h] - lo[h] * ue
        if p + 1 < BLK // SUB:
            n0 = r0 + SUB
            hi, lw = split(u[r0:n0, :])
            left = jnp.concatenate([hi, hi, lw, lw], axis=0)[:, 0:BLK]
            right = jnp.concatenate([hi, lw, hi, lw], axis=0)
            upd = lax.dot_general(left, right, (((0,), (0,)), ((), ())), preferred_element_type=F32)
            w[n0:BLK, :] = w[n0:BLK, :] - upd[n0:BLK, :]


def chol_kernel(nb, a_ref, l_ref, w, pw, u, uh, ul, lh, ll):
    ii = lax.broadcasted_iota(jnp.int32, (BLK, BLK), 0)
    jj = lax.broadcasted_iota(jnp.int32, (BLK, BLK), 1)
    eye = jnp.where(ii == jj, 1.0, 0.0).astype(F32)

    where = gram_places()

    def step(k, carry):
        for q in range(nb):
            @pl.when(k == q)
            def _(q=q):
                c0 = q * BLK
                width = (nb - q) * BLK
                if q:
                    s = dot3(lh[c0:c0 + BLK, 0:c0], ll[c0:c0 + BLK, 0:c0], uh[0:c0, c0:], ul[0:c0, c0:])
                for j in range(q, nb):
                    owner, slot = where[q, j]
                    blk = a_ref[owner, slot * BLK:(slot + 1) * BLK, :]
                    if q:
                        o = (j - q) * BLK
                        blk = blk - s[:, o:o + BLK]
                    if j == q:
                        w[:, 0:BLK] = blk
                    else:
                        pw[:, (j - 1) * BLK:j * BLK] = blk
        w[:, BLK:2 * BLK] = eye
        factor_diagonal(w, u)
        for q in range(nb):
            @pl.when(k == q)
            def _(q=q):
                c0 = q * BLK
                l_ref[c0:c0 + BLK, c0:c0 + BLK] = jnp.where(ii <= jj, u[:, 0:BLK], 0.0).T
                for j in range(q + 1, nb):
                    l_ref[c0:c0 + BLK, j * BLK:(j + 1) * BLK] = jnp.zeros((BLK, BLK), F32)
                if q + 1 < nb:
                    ih, il = split(u[:, BLK:2 * BLK])
                    ph, plo = split(pw[:, c0:])
                    res = dot3(ih, il, ph, plo)
                    rh, rl = split(res)
                    uh[c0:c0 + BLK, c0 + BLK:] = rh
                    ul[c0:c0 + BLK, c0 + BLK:] = rl
                    for j in range(q + 1, nb):
                        o = (j - q - 1) * BLK
                        t = res[:, o:o + BLK].T
                        l_ref[j * BLK:(j + 1) * BLK, c0:c0 + BLK] = t
                        th, tl = split(t)
                        lh[j * BLK:(j + 1) * BLK, c0:c0 + BLK] = th
                        ll[j * BLK:(j + 1) * BLK, c0:c0 + BLK] = tl
        return carry

    lax.fori_loop(0, nb, step, 0)


def cholesky_blocks(a, n):
    nb = n // BLK
    return pl.pallas_call(
        functools.partial(chol_kernel, nb),
        out_shape=jax.ShapeDtypeStruct((n, n), F32),
        in_specs=[pl.BlockSpec(memory_space=pltpu.VMEM)],
        out_specs=pl.BlockSpec(memory_space=pltpu.VMEM),
        scratch_shapes=[
            pltpu.VMEM((BLK, 2 * BLK), F32),
            pltpu.VMEM((BLK, n - BLK), F32),
            pltpu.VMEM((BLK, 2 * BLK), F32),
            pltpu.VMEM((n, n), BF), pltpu.VMEM((n, n), BF),
            pltpu.VMEM((n, n), BF), pltpu.VMEM((n, n), BF),
        ],
        compiler_params=pltpu.CompilerParams(vmem_limit_bytes=40 * 2**20),
        name="block_cholesky",
    )(a)


def wrap(v, n):
    return lax.rem(v + n, n)


def hadamard_signs(rows, columns):
    both = jnp.bitwise_and(
        lax.broadcasted_iota(jnp.int32, (rows, columns), 0),
        lax.broadcasted_iota(jnp.int32, (rows, columns), 1),
    )
    shift = 8
    while shift:
        both = jnp.bitwise_xor(both, jnp.right_shift(both, shift))
        shift //= 2
    return (1 - 2 * jnp.bitwise_and(both, 1)).astype(F32)


def place():
    z, x, c = (lax.axis_index(a) for a in ("rows", "sub_0", "sub_1"))
    return z, x, c, 2 * x + c


def remote(src, dst, send, recv, **where):
    return pltpu.make_async_remote_copy(
        src_ref=src, dst_ref=dst, send_sem=send, recv_sem=recv,
        device_id=where, device_id_type=pl.DeviceIdType.MESH,
    )


def signal(sem, **where):
    pl.semaphore_signal(sem, inc=1, device_id=where, device_id_type=pl.DeviceIdType.MESH)


def sub_step(k, x, c):
    far = jnp.bitwise_xor(k // 2, k // 4)
    return wrap(x + far, SUB0), wrap(x - far, SUB0), lax.rem(c + lax.rem(k, 2), 2)


def exchange_and_mix(x_ref, sg_ref, recv, sgall, hmat, tab, own_sem, sends, recvs, sgs, sgr):
    z, x, c, s_me = place()
    rows = x_ref.shape[0]

    def column(s):
        return x_ref.at[:, pl.ds(pl.multiple_of(s * BLK, BLK), BLK)]

    def data(k):
        to, src, core = sub_step(k, x, c)
        return remote(column(2 * to + core), recv.at[s_me], sends.at[k], recvs.at[k],
                      sub_0=to, sub_1=core), 2 * src + core

    def signs(k):
        to, src, core = sub_step(k, x, c)
        return remote(sg_ref, sgall.at[s_me], sgs.at[k], sgr.at[k], sub_0=to, sub_1=core)

    def start(k, carry):
        signs(k).start()
        data(k)[0].start()
        return carry

    own = pltpu.make_async_copy(column(s_me), recv.at[s_me], own_sem)
    own.start()
    lax.fori_loop(1, 8, start, 0)
    sgall[s_me] = sg_ref[...]
    base = hadamard_signs(BLK, BLK)
    for a in range(rows // BLK):
        for b in range(rows // BLK):
            sign = -1.0 if bin(a & b).count("1") % 2 else 1.0
            hmat[a * BLK:(a + 1) * BLK, b * BLK:(b + 1) * BLK] = (base * sign).astype(BF)

    def transform(s):
        left = hmat[...] * sgall[s].astype(BF)
        hi, lo = split(recv[s])
        both = jnp.concatenate([hi, lo], axis=1)
        res = jnp.dot(left, both, preferred_element_type=F32)
        tab[pl.ds(pl.multiple_of(s * rows, rows), rows), :] = res[:, :BLK] + res[:, BLK:]

    own.wait()
    transform(s_me)

    def arrive(k, carry):
        copy, s = data(k)
        signs(k).wait_recv()
        copy.wait_recv()
        transform(s)
        return carry

    lax.fori_loop(1, 8, arrive, 0)

    def mix(q, carry):
        at = [pl.ds(pl.multiple_of(s * rows + 8 * q, 8), 8) for s in range(8)]
        v = [tab[at[s], :] for s in range(8)]
        for bit in (1, 2, 4):
            v = [v[s ^ bit] - v[s] if s & bit else v[s] + v[s ^ bit] for s in range(8)]
        for s in range(8):
            w = v[s] * (1.0 / 256.0)
            tab[at[s], :] = w
            tab[pl.ds(pl.multiple_of((8 + s) * rows + 8 * q, 8), 8), :] = -w
        return carry

    lax.fori_loop(0, rows // 8, mix, 0)

    def finish(k, carry):
        data(k)[0].wait_send()
        signs(k).wait_send()
        return carry

    lax.fori_loop(1, 8, finish, 0)


def ring_sum(length, pieces, own_term, last, bufs, sems):
    z, x, c, s_me = place()
    up = 1 - 2 * c
    send_buf, recv_buf = bufs
    sent, got = sems
    half = length // 2

    def copy(w, t, h):
        to = wrap(z + up * (1 - 2 * w), length)
        return remote(send_buf.at[w, t, h], recv_buf.at[w, t, h],
                      sent.at[w, t, h], got.at[w, t, h], rows=to)

    def dest(w, t):
        return wrap(z + up * (1 - 2 * w) * (half - w - t), length)

    for h in range(pieces):
        for w in range(2):
            own_term(dest(w, 0), h, send_buf.at[w, 0, h])
            copy(w, 0, h).start()

    def advance(w, t):
        for h in range(pieces):
            own_term(dest(w, t), h, send_buf.at[w, t, h])
        for h in range(pieces):
            copy(w, t - 1, h).wait_recv()
            send_buf[w, t, h] = send_buf[w, t, h] + recv_buf[w, t - 1, h]
            copy(w, t, h).start()

    def step(t, carry):
        advance(0, t)
        advance(1, t)
        return carry

    lax.fori_loop(1, half - 1, step, 0)
    advance(0, half - 1)
    for h in range(pieces):
        own_term(z, h, last.at[h])
    for h in range(pieces):
        copy(1, half - 2, h).wait_recv()
        last[h] = last[h] + recv_buf[1, half - 2, h]
        copy(0, half - 1, h).wait_recv()
        last[h] = last[h] + recv_buf[0, half - 1, h]

    def finish(t, carry):
        for w in range(2):
            for h in range(pieces):
                copy(w, t, h).wait_send()
        return carry

    lax.fori_loop(0, half - 1, finish, 0)
    for h in range(pieces):
        copy(0, half - 1, h).wait_send()


def ring_gather(length, rows, buf, sems):
    z, x, c, s_me = place()
    up = 1 - 2 * c
    sent, got = sems
    half = length // 2

    def copy(w, t):
        way = up * (1 - 2 * w)
        piece = wrap(z - way * t, length)
        part = buf.at[pl.ds(pl.multiple_of(piece * rows, 8), rows), :]
        return remote(part, part, sent.at[w, t], got.at[w, t], rows=wrap(z + way, length))

    def arrived(w, t):
        way = up * (1 - 2 * w)
        piece = wrap(z - way * (t + 1), length)
        part = buf.at[pl.ds(pl.multiple_of(piece * rows, 8), rows), :]
        remote(part, part, sent.at[w, t], got.at[w, t], rows=wrap(z + way, length)).wait_recv()

    copy(0, 0).start()
    copy(1, 0).start()

    def step(t, carry):
        for w in range(2):
            arrived(w, t - 1)
            copy(w, t).start()
        return carry

    lax.fori_loop(1, half - 1, step, 0)
    arrived(0, half - 2)
    copy(0, half - 1).start()
    arrived(1, half - 2)
    arrived(0, half - 1)

    def finish(t, carry):
        for w in range(2):
            copy(w, t).wait_send()
        return carry

    lax.fori_loop(0, half - 1, finish, 0)
    copy(0, half - 1).wait_send()


def gram_pair(slot, x, c):
    s = 2 * x + c
    right, left = 2 * ((x + 1) % SUB0), 2 * ((x + SUB0 - 1) % SUB0)
    return [
        (s, s), (s, right), (s, right + 1),
        (left + c, right + (c + x // 2) % 2),
        (2 * x, 2 * x + 1),
    ][slot]


def gram_places():
    where = {}
    for x in range(SUB0):
        for c in range(2):
            for slot in range(SLOTS):
                a, b = gram_pair(slot, x, c)
                where.setdefault((min(a, b), max(a, b)), (2 * x + c, slot))
    return where


def share_picks(picks, sems):
    z, x, c, s_me = place()
    sent, got = sems
    steps = [(0, 1), (1, 0), (1, 1), (3, 0), (3, 1)]
    copies = []
    for k, (far, flip) in enumerate(steps):
        to, core = wrap(x + far, SUB0), lax.rem(c + flip, 2)
        cp = remote(picks.at[s_me], picks.at[s_me], sent.at[k], got.at[k], sub_0=to, sub_1=core)
        cp.start()
    for k, (far, flip) in enumerate(steps):
        src, core = 2 * wrap(x - far, SUB0) + lax.rem(c + flip, 2), lax.rem(c + flip, 2)
        cp = remote(picks.at[src], picks.at[src], sent.at[k], got.at[k],
                    sub_0=wrap(x + far, SUB0), sub_1=core)
        copies.append(cp)
        cp.wait_recv()
    for cp in copies:
        cp.wait_send()


def gram_parts(picks, parts, scale):
    z, x, c, s_me = place()
    tdot = lambda a, b: lax.dot_general(a, b, (((0,), (0,)), ((), ())), preferred_element_type=F32)
    for slot in range(SLOTS):
        a, b = gram_pair(slot, x, c)
        ah, al = split(picks[jnp.minimum(a, b)])
        bh, bl = split(picks[jnp.maximum(a, b)])
        parts[slot * BLK:(slot + 1) * BLK, :] = (tdot(ah, bh) + (tdot(ah, bl) + tdot(al, bh))) * scale


def share_blocks(total, out_ref, sems):
    z, x, c, s_me = place()
    sent, got, dsent, dgot = sems
    rows = total.shape[0]
    half = rows // 2
    cut = [pl.ds(0, half), pl.ds(half, half)]
    left, right = wrap(x - 1, SUB0), wrap(x + 1, SUB0)
    across = wrap(x + 2, SUB0)

    def hop(way, k, owner, part):
        ref = out_ref.at[2 * owner + c, cut[part]]
        return remote(ref, ref, sent.at[way, k], got.at[way, k], sub_0=right if way == 0 else left)

    def over(k, owner, part):
        ref = out_ref.at[2 * owner + c, cut[part]]
        return remote(ref, ref, dsent.at[k], dgot.at[k], sub_1=1 - c)

    def came(k, owner, part):
        ref = out_ref.at[2 * owner + (1 - c), cut[part]]
        return remote(ref, ref, dsent.at[k], dgot.at[k], sub_1=1 - c)

    out_ref[s_me] = total[...]
    for way in range(2):
        hop(way, 0, x, way).start()
    for way in range(2):
        hop(way, 1, x, 1 - way).start()
    for part in range(2):
        over(part, x, part).start()
    back = [left, right]
    for way in range(2):
        hop(way, 0, back[way], way).wait_recv()
        hop(way, 2, back[way], way).start()
        over(2 + way, back[way], way).start()
    for way in range(2):
        hop(way, 1, back[way], 1 - way).wait_recv()
        over(4 + way, back[way], 1 - way).start()
    for way in range(2):
        hop(way, 2, across, way).wait_recv()
        over(6 + way, across, way).start()
    order = [(0, x, 0), (1, x, 1), (2, left, 0), (3, right, 1), (4, left, 1), (5, right, 0),
             (6, across, 0), (7, across, 1)]
    for k, owner, part in order:
        came(k, owner, part).wait_recv()
    for way in range(2):
        hop(way, 0, x, way).wait_send()
        hop(way, 1, x, 1 - way).wait_send()
        hop(way, 2, back[way], way).wait_send()
    for k, owner, part in order:
        over(k, owner, part).wait_send()


def sketch_kernel(length, scale, stop, x_ref, sg_ref, idx_ref, out_ref,
                  recv, sgall, hmat, tab, pbuf_s, pbuf_r, last, picks, parts, gbuf_s, gbuf_r,
                  glast, total, own_sem, a_s, a_r, g_s, g_r, p_s, p_r, q_s, q_r, e_s, e_r,
                  w_s, w_r, h_s, h_r, d_s, d_r):
    z, x, c, s_me = place()
    barrier = pltpu.get_barrier_semaphore()
    for k in range(1, 8):
        signal(barrier, sub_0=wrap(x + k // 2, SUB0), sub_1=lax.rem(c + k % 2, 2))
    for far in (1, length - 1):
        signal(barrier, rows=wrap(z + far, length))
    pl.semaphore_wait(barrier, 9)

    exchange_and_mix(x_ref, sg_ref, recv, sgall, hmat, tab, own_sem, a_s, a_r, g_s, g_r)
    pieces, rows = last.shape[0], last.shape[1]

    def gather(dest, part, ref):
        def some(q, carry):
            for e in range(8):
                j = idx_ref[dest, part * rows + 8 * q + e]
                ref[pl.ds(8 * q + e, 1), :] = tab[pl.ds(j, 1), :]
            return carry

        lax.fori_loop(0, rows // 8, some, 0)

    ring_sum(length, pieces, gather, last, (pbuf_s, pbuf_r), (p_s, p_r))
    for h in range(pieces):
        picks[s_me, h * rows:(h + 1) * rows, :] = last[h]
    share_picks(picks, (e_s, e_r))
    gram_parts(picks, parts, scale)
    small = glast.shape[1]

    def own_part(dest, part, ref):
        ref[...] = parts[pl.ds(pl.multiple_of(dest * small, 8), small), :]

    ring_sum(length, 1, own_part, glast, (gbuf_s, gbuf_r), (q_s, q_r))
    total[pl.ds(pl.multiple_of(z * small, 8), small), :] = glast[0]
    ring_gather(length, small, total, (w_s, w_r))
    share_blocks(total, out_ref, (h_s, h_r, d_s, d_r))


def sketch_gram(matrix, signs, index, scale):
    rows, columns = matrix.shape
    length, samples = index.shape
    half = length // 2
    pieces = PIECES
    small = SLOTS * BLK // length
    dma = pltpu.SemaphoreType.DMA
    return pl.pallas_call(
        functools.partial(sketch_kernel, length, scale, 0),
        out_shape=jax.ShapeDtypeStruct((columns // BLK, SLOTS * BLK, BLK), F32),
        in_specs=[
            pl.BlockSpec(memory_space=pl.ANY),
            pl.BlockSpec(memory_space=pltpu.VMEM),
            pl.BlockSpec(memory_space=pltpu.SMEM),
        ],
        out_specs=pl.BlockSpec(memory_space=pltpu.VMEM),
        scratch_shapes=[
            pltpu.VMEM((8, rows, BLK), F32), pltpu.VMEM((8, 1, rows), F32),
            pltpu.VMEM((rows, rows), BF), pltpu.VMEM((16 * rows, BLK), F32),
            pltpu.VMEM((2, half, pieces, samples // pieces, BLK), F32),
            pltpu.VMEM((2, half, pieces, samples // pieces, BLK), F32),
            pltpu.VMEM((pieces, samples // pieces, BLK), F32),
            pltpu.VMEM((8, samples, BLK), F32),
            pltpu.VMEM((SLOTS * BLK, BLK), F32),
            pltpu.VMEM((2, half, 1, small, BLK), F32), pltpu.VMEM((2, half, 1, small, BLK), F32),
            pltpu.VMEM((1, small, BLK), F32), pltpu.VMEM((SLOTS * BLK, BLK), F32),
            dma, dma((8,)), dma((8,)), dma((8,)), dma((8,)),
            dma((2, half, pieces)), dma((2, half, pieces)),
            dma((2, half, 1)), dma((2, half, 1)), dma((5,)), dma((5,)),
            dma((2, half)), dma((2, half)), dma((2, 3)), dma((2, 3)), dma((8,)), dma((8,)),
        ],
        compiler_params=pltpu.CompilerParams(
            collective_id=0, has_side_effects=True, vmem_limit_bytes=48 * 2**20),
        name="sketch_gram",
    )(matrix, signs, index)


def body(matrix, sign_bits, samples):
    rows, columns = matrix.shape
    length = lax.axis_size("rows")
    z = lax.axis_index("rows")
    signs = (2 * sign_bits - 1).astype(F32).reshape(1, rows)
    local = 8 * rows
    high = jnp.bitwise_and(samples // local, z)
    shift = 8
    while shift:
        high = jnp.bitwise_xor(high, jnp.right_shift(high, shift))
        shift //= 2
    index = samples % local + local * jnp.bitwise_and(high, 1)
    blocks = sketch_gram(matrix, signs, index.reshape(length, -1), 1.0 / samples.shape[0])
    return cholesky_blocks(blocks, columns)


def solution(mesh):
    torus = Mesh(
        mesh.devices.reshape(mesh.shape["groups"], mesh.shape["rows"], SUB0, 2),
        ("groups", "rows", "sub_0", "sub_1"),
    )
    in_specs = (P(GROUPS_ROWS_SUB, None), P(GROUPS_ROWS_SUB), P("groups"))
    return jax.shard_map(
        body, mesh=torus, in_specs=in_specs, out_specs=P("groups", None), check_vma=False)
```
